32 devices in a mesh: elem: 4 (over y, x), pulse: 8 (over z, core).
Axes of the slice: x: 2, y: 2, z: 4, core: 2. Of those that a mesh axis runs over, the one named last changes fastest.
Arguments:
- echoes: bfloat16 [2, 2048, 256, 256], P(None, 'elem', 'pulse'), may hold values from -6 to 6
- keep_mask: int32 [256, 8], P('pulse'), may hold values from 0 to 1, as said below
- steer_index: int32 [512], replicated, may hold values from 0 to 1023
- element_position: float32 [2048], replicated, may hold values from 0 to 1024
- element_gain: float32 [2, 2048], replicated, may hold values from -4 to 4
- steer_sines: float32 [1024], replicated, may hold values from -1 to 1
Outputs:
- doppler_power: float32 [512, 256, 256], P('pulse', None, 'elem')
The draws below stay inside these ranges and needn't reach their ends.
Inputs may be any that keep to these rules, and one draw needn't show every extreme that they name: `keep_mask`: in each masking block, each aligned run of 32 pulses keeps at most 24 pulses, and at least one; in every masking block some run keeps exactly 24.
All inputs are finite; a program needn't handle non-finite values.
Results may differ from the reference program's by a relative error of at most 0.005.
Values may be sent and summed in bfloat16 or wider, within the bound.
No kernel may reach another device: no remote copies, remote signals or barrier semaphores. Data moves between devices by JAX's collectives and lax.ppermute only.
A program may use at most 128 MiB of HBM per device.

```python
import math
import jax
import jax.numpy as jnp
from jax import lax

E = 2048
B = 512
P_SIZE = 256
NV = 1024
RBLK = 32
R = 256
NRB = 8
PL = 32
KEPT = 24


def draw_keep_mask(key, part):
    count_key, top_key, order_key = jax.random.split(jax.random.fold_in(key, 7), 3)
    blocks = R // RBLK
    runs = P_SIZE // PL
    counts = jax.random.randint(count_key, (runs, blocks), max(1, PL // 4), KEPT + 1)
    top = jax.random.randint(top_key, (blocks,), 0, runs)
    counts = jnp.where(jnp.arange(runs, dtype=jnp.int32)[:, None] == top[None, :], KEPT, counts)
    order_keys = jax.random.split(order_key, runs * blocks)
    ranks = jax.vmap(lambda one: jax.random.permutation(one, PL))(order_keys)
    ranks = jnp.transpose(ranks.reshape(runs, blocks, PL), (0, 2, 1))
    kept = ranks < counts[:, None, :]
    return kept.reshape(P_SIZE, blocks).astype(jnp.int32)


def plant(result, rng, low, high):
    index_at = [jax.random.randint(jax.random.fold_in(rng, axis), (), 0, length) for axis, length in enumerate(result.shape)]
    main_axis = result.shape.index(max(result.shape))
    neighbour = index_at[:main_axis] + [(index_at[main_axis] + 1) % result.shape[main_axis]] + index_at[main_axis + 1:]
    return result.at[tuple(index_at)].set(low).at[tuple(neighbour)].set(high)


def block_levels(own_key, dims, cuts, least, high):
    gain, own = 1.0, jax.random.fold_in(own_key, 6)
    for position, shards_of in cuts:
        draws = jnp.exp(jax.random.uniform(jax.random.fold_in(own, position), (shards_of,), jnp.float32, least / len(cuts), high / len(cuts)))
        gain = gain * jnp.repeat(draws, dims[position] // shards_of).reshape([-1 if axis == position else 1 for axis in range(len(dims))])
    return gain


def noise(stream_key, dims, scale, limit, shards=(), held_as=jnp.bfloat16):
    gain = block_levels(stream_key, dims, shards, -0.22, 0.18) if shards else 1.0
    result = jax.random.normal(stream_key, dims, jnp.float32) * scale * gain
    return jnp.minimum(jnp.maximum(result, -limit), limit).astype(held_as)


def setup_inputs(seed: int = 0) -> dict:
    seeds = jax.random.split(jax.random.key(seed), 7)
    echoes = noise(seeds[0], (2, E, P_SIZE, R), 1.0, 6.0, ((1, 4), (2, 8)))
    keep_mask = draw_keep_mask(jax.random.fold_in(seeds[6], 71), 0)
    steer_index = plant(jax.random.randint(seeds[2], (B,), 0, NV), jax.random.fold_in(seeds[2], 1), 0, NV - 1).astype(jnp.int32)
    element_position = jnp.clip(jax.random.uniform(seeds[3], (E,), jnp.float32, 0.0, 1024.0), 0.0, 1024.0)
    element_gain = noise(seeds[4], (2, E), 1.0, 4.0, (), jnp.float32)
    steer_sines = jnp.clip(jax.random.uniform(seeds[5], (NV,), jnp.float32, -1.0, 1.0), -1.0, 1.0)
    return {"echoes": echoes, "keep_mask": keep_mask, "steer_index": steer_index, "element_position": element_position, "element_gain": element_gain, "steer_sines": steer_sines}


def steering(element_position, element_gain, sines):
    phase = 2.0 * math.pi * element_position[:, None] * sines[None, :]
    cosine = jnp.cos(phase)
    sine = jnp.sin(phase)
    factor = 1.0 / math.sqrt(E)
    real = (element_gain[0][:, None] * cosine + element_gain[1][:, None] * sine) * factor
    imag = (element_gain[1][:, None] * cosine - element_gain[0][:, None] * sine) * factor
    return (real.astype(jnp.bfloat16), imag.astype(jnp.bfloat16))

def tables(count):
    index = jnp.arange(count, dtype=jnp.int32)
    angle = 2.0 * math.pi * (index[:, None] * index[None, :] % count).astype(jnp.float32) / count
    taper = 0.54 - 0.46 * jnp.cos(2.0 * math.pi * index.astype(jnp.float32) / (count - 1))
    taper = taper / math.sqrt(count)
    cos_table = jnp.cos(angle) * taper[None, :]
    sin_table = jnp.sin(angle) * taper[None, :]
    upper = jnp.concatenate((cos_table, sin_table), axis=1)
    lower = jnp.concatenate((-sin_table, cos_table), axis=1)
    transform = jnp.concatenate((upper, lower), axis=0)
    high = transform.astype(jnp.bfloat16)
    low = (transform - high.astype(jnp.float32)).astype(jnp.bfloat16)
    return (high, low)

def contract(left, right):
    return lax.dot_general(left, right, (((0,), (0,)), ((), ())), preferred_element_type=jnp.float32)

def beamform(weight_re, weight_im, sample_re, sample_im):
    real = contract(weight_re, sample_re) - contract(weight_im, sample_im)
    imag = contract(weight_re, sample_im) + contract(weight_im, sample_re)
    return (real, imag)

def spectrum(high, low, beam_re, beam_im):
    count = beam_re.shape[1]
    total = jnp.zeros((beam_re.shape[0], 2 * count, beam_re.shape[2]), jnp.float32)
    for table in (high, low):
        left = table[:, :count].astype(jnp.float32)
        right = table[:, count:].astype(jnp.float32)
        total = total + jnp.einsum('fp,bpn->bfn', left, beam_re.astype(jnp.float32), precision=lax.Precision.HIGHEST)
        total = total + jnp.einsum('fp,bpn->bfn', right, beam_im.astype(jnp.float32), precision=lax.Precision.HIGHEST)
    real = total[:, :count]
    imag = total[:, count:]
    return real * real + imag * imag

def reference(echoes, keep_mask, steer_index, element_position, element_gain, steer_sines):
    sines = steer_sines[steer_index]
    weight_re, weight_im = steering(element_position, element_gain, sines)
    high, low = tables(P_SIZE)

    def block(index):
        start = (index * RBLK).astype(jnp.int32)
        piece = lax.dynamic_slice_in_dim(echoes, start, RBLK, 3)
        keeper = lax.dynamic_slice_in_dim(keep_mask, index.astype(jnp.int32), 1, 1)
        keeper = keeper.astype(jnp.bfloat16)[None, None, :, :]
        piece = piece * keeper
        flat = piece.reshape(2, E, P_SIZE * RBLK)
        real, imag = beamform(weight_re, weight_im, flat[0], flat[1])
        real = real.astype(jnp.bfloat16).reshape(B, P_SIZE, RBLK)
        imag = imag.astype(jnp.bfloat16).reshape(B, P_SIZE, RBLK)
        return spectrum(high, low, real, imag)
    stacked = lax.map(block, jnp.arange(NRB, dtype=jnp.int32))
    return jnp.transpose(stacked, (1, 2, 0, 3)).reshape(B, P_SIZE, NRB * RBLK)
```

```python
import functools
import math

import jax
import jax.numpy as jnp
from jax import lax
from jax.experimental import pallas as pl
from jax.experimental.pallas import tpu as pltpu
from jax.sharding import PartitionSpec as P


E = 2048
P_SIZE = 256
RBLK = 32
LANES = 128
TILE = 16
PAIRS = 4


def tables(count):
    index = jnp.arange(count, dtype=jnp.int32)
    angle = 2.0 * math.pi * (index[:, None] * index[None, :] % count).astype(jnp.float32) / count
    taper = 0.54 - 0.46 * jnp.cos(2.0 * math.pi * index.astype(jnp.float32) / (count - 1))
    taper = taper / math.sqrt(count)
    cos_table = jnp.cos(angle) * taper[None, :]
    sin_table = jnp.sin(angle) * taper[None, :]
    upper = jnp.concatenate((cos_table, sin_table), axis=1)
    lower = jnp.concatenate((-sin_table, cos_table), axis=1)
    transform = jnp.concatenate((upper, lower), axis=0)
    high = transform.astype(jnp.bfloat16)
    low = (transform - high.astype(jnp.float32)).astype(jnp.bfloat16)
    return (high, low)


def local_weight(position, gain, sines):
    phase = (2.0 * math.pi * position)[None, :] * sines[:, None]
    cosine = jnp.cos(phase)
    sine = jnp.sin(phase)
    factor = 1.0 / math.sqrt(E)
    real = ((gain[0][None, :] * cosine + gain[1][None, :] * sine) * factor).astype(jnp.bfloat16)
    imag = ((gain[1][None, :] * cosine - gain[0][None, :] * sine) * factor).astype(jnp.bfloat16)
    upper = jnp.concatenate((real, -imag), axis=1)
    lower = jnp.concatenate((imag, real), axis=1)
    return jnp.concatenate((upper, lower), axis=0)


def slot_sources(mask, slots):
    length = mask.shape[-2]
    zeroed = 1 - mask
    index = jnp.arange(length, dtype=jnp.int32)
    earlier = (index[:, None] > index[None, :]).astype(jnp.int32)
    before = jnp.sum(earlier[:, :, None] * zeroed[..., None, :, :], axis=-2)
    out = (zeroed == 1) & (before < length - slots)
    rank = index[:, None] - jnp.minimum(before, length - slots)
    ids = jnp.arange(slots, dtype=jnp.int32)
    hit = (rank[..., None, :, :] == ids[:, None, None]) & jnp.logical_not(out)[..., None, :, :]
    return hit


def swap_matrix():
    row = jnp.arange(TILE * TILE, dtype=jnp.int32)
    source = (row % TILE) * TILE + row // TILE
    return (source[:, None] == row[None, :]).astype(jnp.bfloat16)


def gather_kernel(slots, per_block, src_ref, swap_ref, x_ref, out_ref, turned):
    elems, pulses, cells = x_ref.shape[1:]
    pstep = min(pulses, TILE)
    estep = TILE * TILE // pstep
    blocks = cells // per_block
    for start in range(0, elems, estep):
        for first in range(0, pulses, pstep):
            block = x_ref[0, start : start + estep, first : first + pstep, :]
            block = block.reshape(estep * pstep, cells)
            rows = jnp.dot(swap_ref[...], block, preferred_element_type=jnp.float32)
            rows = rows.astype(jnp.bfloat16).reshape(pstep, estep, cells)
            turned[first : first + pstep, start : start + estep, :] = rows
    lane = lax.broadcasted_iota(jnp.int32, (elems, LANES), 1) // per_block

    def slot(s, carry):
        for column in range(cells // LANES):
            span = slice(column * LANES, (column + 1) * LANES)
            first = column * (LANES // per_block)
            value = turned[src_ref[s * blocks + first], :, span]
            for piece in range(1, LANES // per_block):
                other = turned[src_ref[s * blocks + first + piece], :, span]
                value = jnp.where(lane >= piece, other, value)
            out_ref[s, 0, :, span] = value
        return carry

    lax.fori_loop(0, slots, slot, 0)


def gather_slots(echoes, sources, slots, per_block):
    parts, elems, pulses, cells = echoes.shape
    chunk = min(elems, 128)
    pstep = min(pulses, TILE)
    estep = TILE * TILE // pstep
    row = jnp.arange(TILE * TILE, dtype=jnp.int32)
    source = (row % estep) * pstep + row // estep
    swap = (source[:, None] == row[None, :]).astype(jnp.bfloat16)
    return pl.pallas_call(
        functools.partial(gather_kernel, slots, per_block),
        out_shape=jax.ShapeDtypeStruct((slots, parts, elems, cells), jnp.bfloat16),
        grid_spec=pltpu.PrefetchScalarGridSpec(
            num_scalar_prefetch=1,
            grid=(parts, elems // chunk),
            in_specs=[
                pl.BlockSpec(swap.shape, lambda c, e, src: (0, 0)),
                pl.BlockSpec((1, chunk, pulses, cells), lambda c, e, src: (c, e, 0, 0)),
            ],
            out_specs=pl.BlockSpec((slots, 1, chunk, cells), lambda c, e, src: (0, c, e, 0)),
            scratch_shapes=[pltpu.VMEM((pulses, chunk, cells), jnp.bfloat16)],
        ),
        compiler_params=pltpu.CompilerParams(vmem_limit_bytes=40 * 1024 * 1024),
        cost_estimate=pl.CostEstimate(
            flops=2 * echoes.size * TILE * TILE, bytes_accessed=4 * echoes.size, transcendentals=0
        ),
        name="gather_slots",
    )(sources, swap, echoes)


def beam_kernel(groups, orders, me_ref, w_ref, *refs):
    xs, outs = refs[: len(orders)], refs[len(orders) :]
    bits = len(orders[0])
    flags = [me_ref[bit] == 1 for bit in range(bits)]
    for half, order in enumerate(orders):
        keep_ref, send_ref = outs[2 * half], outs[2 * half + 1]
        total = jnp.dot(w_ref[...], xs[half][0], preferred_element_type=jnp.float32)
        beams = total.shape[0] // 2
        cells = total.shape[1] // groups
        shape = (keep_ref.shape[1], keep_ref.shape[3], 2 * cells)
        low_lanes = lax.broadcasted_iota(jnp.int32, (beams, LANES), 1) < cells
        blocks = []
        for column in range(total.shape[1] // LANES):
            span = slice(column * LANES, (column + 1) * LANES)
            real, imag = total[:beams, span], total[beams:, span]
            even = jnp.where(low_lanes, real, pltpu.roll(imag, cells, 1))
            odd = jnp.where(low_lanes, pltpu.roll(real, cells, 1), imag)
            blocks += [even.astype(jnp.bfloat16), odd.astype(jnp.bfloat16)]
        for bit in range(bits):
            blocks = [
                jnp.where(flags[bit], blocks[g ^ (1 << bit)], blocks[g]) for g in range(groups)
            ]
        for away in range(groups):
            place = 0
            for bit in order:
                place = 2 * place + ((away >> bit) & 1)
            ref = send_ref if place >= groups // 2 else keep_ref
            ref[place % (groups // 2), :, 0] = blocks[away].reshape(shape)


def form_beams(mine, weight, gathered, first, count, orders, owners, groups):
    slots, depth, cells = gathered.shape
    beams = weight.shape[0] // 2
    shape = (groups // 2, owners, count, beams // owners, 2 * (cells // groups))
    block = shape[:2] + (1,) + shape[3:]
    starts = [first + half * count for half in range(len(orders))]
    outs = [jax.ShapeDtypeStruct(shape, jnp.bfloat16)] * (2 * len(orders))
    return pl.pallas_call(
        functools.partial(beam_kernel, groups, orders),
        out_shape=outs,
        grid_spec=pltpu.PrefetchScalarGridSpec(
            num_scalar_prefetch=1,
            grid=(count,),
            in_specs=[pl.BlockSpec(weight.shape, lambda i, me: (0, 0))]
            + [
                pl.BlockSpec((1, depth, cells), functools.partial(lambda at, i, me: (at + i, 0, 0), at))
                for at in starts
            ],
            out_specs=[pl.BlockSpec(block, lambda i, me: (0, 0, i, 0, 0))] * len(outs),
        ),
        compiler_params=pltpu.CompilerParams(vmem_limit_bytes=40 * 1024 * 1024),
        cost_estimate=pl.CostEstimate(
            flops=2 * len(orders) * count * weight.size * cells,
            bytes_accessed=2 * weight.size + 8 * len(orders) * count * depth * cells,
            transcendentals=0,
        ),
        name="form_beams",
    )(mine, weight, *([gathered] * len(orders)))


def doppler_kernel(swap_ref, high_ref, low_ref, *refs):
    ins, out_ref, turned, lines = refs[:-3], refs[-3], refs[-2], refs[-1]
    beams = out_ref.shape[0]
    blocks, parts = lines.shape[0], lines.shape[1]
    per_block = out_ref.shape[1] // blocks
    at = 0
    for ref in ins:
        runs, slots = ref.shape[0], ref.shape[1]
        rows = ref[...].reshape(runs * slots, beams, LANES)
        for first in range(0, runs * slots, TILE):
            piece = rows[first : first + TILE].reshape(TILE * beams, LANES)
            piece = jnp.dot(swap_ref[...], piece, preferred_element_type=jnp.float32)
            turned[:, at : at + TILE, :] = piece.astype(jnp.bfloat16).reshape(beams, TILE, LANES)
            at += TILE
    for beam in range(beams):
        flipped = turned[beam].T
        for part in range(parts):
            for block in range(blocks):
                row = (part * blocks + block) * per_block
                lines[block, part, beam * per_block : (beam + 1) * per_block, :] = flipped[
                    row : row + per_block
                ]
    for block in range(blocks):
        total = None
        for part in range(parts):
            for table in (high_ref, low_ref):
                term = jnp.dot(
                    lines[block, part], table[block, part], preferred_element_type=jnp.float32
                )
                total = term if total is None else total + term
        count = total.shape[1] // 2
        real, imag = total[:, :count], total[:, count:]
        power = (real * real + imag * imag).reshape(beams, per_block, count)
        out_ref[:, block * per_block : (block + 1) * per_block, :] = power


def doppler(pieces, high, low, per_block):
    blocks, parts, columns, width = high.shape
    beams = pieces[0].shape[2]
    row = jnp.arange(TILE * TILE, dtype=jnp.int32)
    source = (row % TILE) * TILE + row // TILE
    swap = (source[:, None] == row[None, :]).astype(jnp.bfloat16)
    whole = lambda shape: pl.BlockSpec(shape, lambda i: (0,) * len(shape))
    cells = blocks * per_block
    return pl.pallas_call(
        doppler_kernel,
        out_shape=jax.ShapeDtypeStruct((beams, cells, width // 2), jnp.float32),
        grid=(beams // TILE,),
        in_specs=[whole(swap.shape), whole(high.shape), whole(low.shape)]
        + [
            pl.BlockSpec((p.shape[0], p.shape[1], TILE, LANES), lambda i: (0, 0, i, 0))
            for p in pieces
        ],
        out_specs=pl.BlockSpec((TILE, cells, width // 2), lambda i: (i, 0, 0)),
        scratch_shapes=[
            pltpu.VMEM((TILE, columns, LANES), jnp.bfloat16),
            pltpu.VMEM((blocks, parts, TILE * per_block, columns), jnp.bfloat16),
        ],
        compiler_params=pltpu.CompilerParams(vmem_limit_bytes=40 * 1024 * 1024),
        cost_estimate=pl.CostEstimate(
            flops=4 * beams * cells * parts * columns * width,
            bytes_accessed=4 * beams * cells * width,
            transcendentals=0,
        ),
        name="doppler",
    )(swap, high, low, *pieces)


def add(left, right):
    return (left.astype(jnp.float32) + right.astype(jnp.float32)).astype(jnp.bfloat16)


def per_device(echoes, keep_mask, steer_index, element_position, element_gain, steer_sines):
    groups, owners = lax.axis_size("elem"), lax.axis_size("pulse")
    parts, elems, pulses, all_cells = echoes.shape
    blocks_all = keep_mask.shape[1]
    per_block = all_cells // blocks_all
    cells = all_cells // groups
    bits = groups.bit_length() - 1
    slots = (3 * pulses + 3) // 4
    me = lax.axis_index("elem")

    hit = slot_sources(keep_mask, slots)
    sources = jnp.sum(
        jnp.where(hit, jnp.arange(pulses, dtype=jnp.int32)[None, :, None], 0), axis=1
    ).reshape(-1)
    gathered = gather_slots(echoes, sources, slots, per_block)
    gathered = gathered.reshape(slots, parts * elems, all_cells)

    choices = jnp.arange(steer_sines.shape[0], dtype=jnp.int32)
    sines = jnp.sum(
        jnp.where(steer_index[:, None] == choices[None, :], steer_sines[None, :], 0.0), axis=1
    )
    position = lax.dynamic_slice_in_dim(element_position, me * elems, elems, 0)
    gain = lax.dynamic_slice_in_dim(element_gain, me * elems, elems, 1)
    weight = local_weight(position, gain, sines)

    mine = jnp.stack([(me >> bit) & 1 for bit in range(bits)]).astype(jnp.int32)
    forward = tuple(range(bits))
    orders = (forward, forward[::-1])
    pairs = min(PAIRS, slots // 2)
    count = slots // (2 * pairs)

    def send(value, bit):
        return lax.ppermute(value, "elem", [(i, i ^ (1 << bit)) for i in range(groups)])

    pieces = []
    summed = []
    for pair in range(pairs):
        own = weight
        if pair >= 2:
            own = lax.optimization_barrier((weight, summed[pair - 2]))[0]
        outs = form_beams(mine, own, gathered, pair * 2 * count, count, orders, owners, groups)
        states = [(outs[0], outs[1]), (outs[2], outs[3])]
        for stage in range(bits):
            for half in range(2):
                keep, away = states[half]
                got = send(away, orders[half][stage])
                if stage == bits - 1:
                    states[half] = add(got, keep)
                else:
                    middle = keep.shape[0] // 2
                    states[half] = (
                        add(got[:middle], keep[:middle]),
                        add(got[middle:], keep[middle:]),
                    )
            if stage == 0:
                summed.append(jax.tree.leaves(states)[0])
        final = jnp.concatenate([state[0] for state in states], axis=1)
        pieces.append(lax.all_to_all(final, "pulse", split_axis=0, concat_axis=0, tiled=True))

    every_mask = lax.all_gather(keep_mask, "pulse", axis=0, tiled=False)
    near = lax.dynamic_slice_in_dim(every_mask, me * (cells // per_block), cells // per_block, 2)
    hits = slot_sources(near, slots)
    hits = hits & (near[:, None] == 1)
    high, low = tables(P_SIZE)
    run_eye = jnp.arange(owners, dtype=jnp.int32)
    order = []
    for pair in range(pairs):
        part = hits[:, pair * 2 * count : (pair + 1) * 2 * count]
        order.append(part.reshape(owners * 2 * count, pulses, -1))
    picks = jnp.concatenate(order, axis=0)
    runs = jnp.concatenate([jnp.repeat(run_eye, 2 * count)] * pairs)
    onehot = (
        (runs[:, None] == run_eye[None, :])[:, :, None, None] & picks[:, None, :, :]
    ).reshape(picks.shape[0], owners * pulses, -1).astype(jnp.bfloat16)

    def chosen(table):
        halves = table.reshape(2 * P_SIZE, 2, P_SIZE)
        return jnp.einsum(
            "fcp,spk->kcsf", halves, onehot, preferred_element_type=jnp.float32
        ).astype(jnp.bfloat16)

    power = doppler(pieces, chosen(high), chosen(low), per_block)
    return jnp.transpose(power, (0, 2, 1))


def solution(mesh):
    placed = (P(None, "elem", "pulse", None), P("pulse", None), P(), P(), P(), P())
    return jax.shard_map(
        per_device, mesh=mesh, in_specs=placed, out_specs=P("pulse", None, "elem"), check_vma=False
    )
```

```python
import functools
import math

import jax
import jax.numpy as jnp
import numpy as np
from jax import lax
from jax.experimental import pallas as pl
from jax.experimental.pallas import tpu as pltpu
from jax.sharding import PartitionSpec as P


E = 2048
P_SIZE = 256
LANES = 128
TILE = 16
READS = 2
VMEM = 60 * 1024 * 1024
SHARES = (3, 3, 3, 3)


def tables(count):
    index = jnp.arange(count, dtype=jnp.int32)
    angle = 2.0 * math.pi * (index[:, None] * index[None, :] % count).astype(jnp.float32) / count
    taper = 0.54 - 0.46 * jnp.cos(2.0 * math.pi * index.astype(jnp.float32) / (count - 1))
    taper = taper / math.sqrt(count)
    cos_table = jnp.cos(angle) * taper[None, :]
    sin_table = jnp.sin(angle) * taper[None, :]
    upper = jnp.concatenate((cos_table, sin_table), axis=1)
    lower = jnp.concatenate((-sin_table, cos_table), axis=1)
    transform = jnp.concatenate((upper, lower), axis=0)
    high = transform.astype(jnp.bfloat16)
    low = (transform - high.astype(jnp.float32)).astype(jnp.bfloat16)
    return (high, low)


def cos_sin(phase):
    turns = jnp.floor(phase * (2.0 / math.pi) + 0.5)
    rest = phase - turns * 1.5703125
    rest = rest - turns * 4.837512969970703e-4
    rest = rest - turns * 7.54978995489188e-8
    square = rest * rest
    sine = ((-1.9515295891e-4 * square + 8.3321608736e-3) * square - 1.6666654611e-1) * square * rest + rest
    cosine = (2.443315711809948e-5 * square - 1.388731625493765e-3) * square + 4.166664568298827e-2
    cosine = cosine * square * square - 0.5 * square + 1.0
    quadrant = turns.astype(jnp.int32)
    odd = (quadrant & 1) == 1
    real = jnp.where(odd, sine, cosine)
    imag = jnp.where(odd, cosine, sine)
    real = jnp.where(((quadrant + 1) & 2) == 2, -real, real)
    imag = jnp.where((quadrant & 2) == 2, -imag, imag)
    return (real, imag)


def weight_kernel(me_ref, sine_ref, position_ref, gain_ref, out_ref):
    phase = (2.0 * math.pi * position_ref[...]) * sine_ref[...]
    cosine, sine = cos_sin(phase)
    factor = 1.0 / math.sqrt(E)
    first, second = gain_ref[0:1, :], gain_ref[1:2, :]
    real = ((first * cosine + second * sine) * factor).astype(jnp.bfloat16)
    imag = (second * cosine - first * sine) * factor
    elems = real.shape[1]
    out_ref[:, :elems] = real
    out_ref[:, elems:] = imag.astype(jnp.bfloat16)


def local_weight(me, position, gain, sines, elems):
    beams = sines.shape[0]
    step = min(beams, 128)
    return pl.pallas_call(
        weight_kernel,
        out_shape=jax.ShapeDtypeStruct((beams, 2 * elems), jnp.bfloat16),
        grid_spec=pltpu.PrefetchScalarGridSpec(
            num_scalar_prefetch=1,
            grid=(beams // step,),
            in_specs=[
                pl.BlockSpec((step, 1), lambda i, me: (i, 0)),
                pl.BlockSpec((1, elems), lambda i, me: (0, me[0])),
                pl.BlockSpec((2, elems), lambda i, me: (0, me[0])),
            ],
            out_specs=pl.BlockSpec((step, 2 * elems), lambda i, me: (i, 0)),
        ),
        compiler_params=pltpu.CompilerParams(vmem_limit_bytes=VMEM // 4),
        cost_estimate=pl.CostEstimate(
            flops=40 * beams * elems, bytes_accessed=8 * beams * elems, transcendentals=0
        ),
        name="weights",
    )(me, sines, position, gain)


def slot_sources(mask, slots):
    length = mask.shape[-2]
    zeroed = 1 - mask
    index = jnp.arange(length, dtype=jnp.int32)
    earlier = (index[:, None] > index[None, :]).astype(jnp.int32)
    before = jnp.sum(earlier[:, :, None] * zeroed[..., None, :, :], axis=-2)
    out = (zeroed == 1) & (before < length - slots)
    rank = index[:, None] - jnp.minimum(before, length - slots)
    ids = jnp.arange(slots, dtype=jnp.int32)
    hit = (rank[..., None, :, :] == ids[:, None, None]) & jnp.logical_not(out)[..., None, :, :]
    return hit


def swap_rows(outer, inner):
    row = np.arange(outer * inner)
    return ((row % outer) * inner + row // outer)[:, None] == row[None, :]


def gather_kernel(first, count, offset, per_block, src_ref, swap_ref, *refs):
    xs, out_ref, turned = refs[:-2], refs[-2], refs[-1]
    depth, pulses, all_cells = xs[0].shape[1:]
    elems = READS * depth
    groups = out_ref.shape[1]
    cells = all_cells // groups
    rows = swap_ref.shape[0]
    estep = rows // pulses
    low = lax.broadcasted_iota(jnp.int32, (rows, LANES), 1) < cells
    for start in range(0, elems, estep):
        for at in range(len(xs) // (2 * READS)):
            real, imag = [
                jnp.dot(
                    swap_ref[...],
                    xs[(2 * at + part) * READS + start // depth][
                        0, start % depth : start % depth + estep
                    ].reshape(rows, all_cells),
                    preferred_element_type=jnp.float32,
                )
                for part in range(2)
            ]
            for column in range(all_cells // LANES):
                span = slice(column * LANES, (column + 1) * LANES)
                re, im = real[:, span], imag[:, span]
                even = jnp.where(low, re, pltpu.roll(im, cells, 1))
                odd = jnp.where(low, pltpu.roll(re, cells, 1), im)
                for side, value in enumerate((even, odd)):
                    turned[
                        at * pulses : (at + 1) * pulses, 2 * column + side, start : start + estep, :
                    ] = value.astype(jnp.bfloat16).reshape(pulses, estep, LANES)
    per_group = cells // per_block
    block = lax.broadcasted_iota(jnp.int32, (elems, LANES), 1) % cells // per_block

    def slot(s, carry):
        for group in range(groups):
            place = (first + s) * (groups * per_group) + group * per_group
            value = turned[src_ref[place] - offset, group]
            for piece in range(1, per_group):
                value = jnp.where(block >= piece, turned[src_ref[place + piece] - offset, group], value)
            out_ref[s, group] = value
        return carry

    lax.fori_loop(0, count, slot, 0)


def gather_slots(echoes, sources, first, count, spare, per_block, groups):
    parts, elems, pulses, all_cells = echoes.shape
    chunk = min(elems, 64)
    pstep = min(pulses, TILE)
    estep = TILE * TILE // pstep
    swap = jnp.asarray(swap_rows(estep, pstep), jnp.bfloat16)
    runs = range(first // pstep, (first + count - 1 + spare) // pstep + 1)
    read = echoes.size * len(runs) * pstep // pulses
    return pl.pallas_call(
        functools.partial(gather_kernel, first, count, runs[0] * pstep, per_block),
        out_shape=jax.ShapeDtypeStruct((count, groups, elems, LANES), jnp.bfloat16),
        grid_spec=pltpu.PrefetchScalarGridSpec(
            num_scalar_prefetch=1,
            grid=(elems // chunk,),
            in_specs=[pl.BlockSpec(swap.shape, lambda e, src: (0, 0))]
            + [
                pl.BlockSpec(
                    (1, chunk // READS, pstep, all_cells),
                    functools.partial(
                        lambda part, read, at, e, src: (part, READS * e + read, at, 0), part, read, run
                    ),
                )
                for run in runs
                for part in range(parts)
                for read in range(READS)
            ],
            out_specs=pl.BlockSpec((count, groups, chunk, LANES), lambda e, src: (0, 0, e, 0)),
            scratch_shapes=[pltpu.VMEM((len(runs) * pstep, groups, chunk, LANES), jnp.bfloat16)],
        ),
        compiler_params=pltpu.CompilerParams(vmem_limit_bytes=VMEM - 4 * 1024 * 1024),
        cost_estimate=pl.CostEstimate(
            flops=2 * read * TILE * TILE, bytes_accessed=4 * read, transcendentals=0
        ),
        name="gather_slots",
    )(sources, swap, *([echoes] * (len(runs) * parts * READS)))


def beam_kernel(groups, orders, me_ref, w_ref, *refs):
    xs, outs = refs[: len(orders)], refs[len(orders) :]
    bits = len(orders[0])
    elems = w_ref.shape[1] // 2
    cells = LANES // 2
    sign = jnp.where(lax.broadcasted_iota(jnp.int32, (elems, LANES), 1) < cells, -1.0, 1.0)
    sign = sign.astype(jnp.bfloat16)
    for half, order in enumerate(orders):
        plain, crossed = [], []
        for place in range(groups):
            away = 0
            for at, bit in enumerate(order):
                away |= ((place >> (bits - 1 - at)) & 1) << bit
            value = xs[half][0, me_ref[0] ^ away]
            plain.append(value)
            crossed.append(pltpu.roll(value, cells, 1) * sign)
        both = jnp.concatenate(
            (jnp.concatenate(plain, axis=1), jnp.concatenate(crossed, axis=1)), axis=0
        )
        total = jnp.dot(w_ref[...], both, preferred_element_type=jnp.float32)
        for place in range(groups):
            ref = outs[2 * half + (1 if place >= groups // 2 else 0)]
            value = total[:, place * LANES : (place + 1) * LANES].astype(jnp.bfloat16)
            ref[place % (groups // 2), :, 0] = value.reshape(ref.shape[1], ref.shape[3], LANES)


def form_beams(me, weight, gathered, first, count, orders, owners):
    _, groups, elems, lanes = gathered.shape
    beams = weight.shape[0]
    shape = (groups // 2, owners, count, beams // owners, lanes)
    block = shape[:2] + (1,) + shape[3:]
    starts = [first + half * count for half in range(len(orders))]
    outs = [jax.ShapeDtypeStruct(shape, jnp.bfloat16)] * (2 * len(orders))
    return pl.pallas_call(
        functools.partial(beam_kernel, groups, orders),
        out_shape=outs,
        grid_spec=pltpu.PrefetchScalarGridSpec(
            num_scalar_prefetch=1,
            grid=(count,),
            in_specs=[pl.BlockSpec(weight.shape, lambda i, me: (0, 0))]
            + [
                pl.BlockSpec(
                    (1, groups, elems, lanes), functools.partial(lambda at, i, me: (at + i, 0, 0, 0), at)
                )
                for at in starts
            ],
            out_specs=[pl.BlockSpec(block, lambda i, me: (0, 0, i, 0, 0))] * len(outs),
        ),
        compiler_params=pltpu.CompilerParams(vmem_limit_bytes=VMEM - 4 * 1024 * 1024),
        cost_estimate=pl.CostEstimate(
            flops=4 * len(orders) * count * weight.size * groups * lanes,
            bytes_accessed=2 * weight.size + 8 * len(orders) * count * groups * elems * lanes,
            transcendentals=0,
        ),
        name="form_beams",
    )(me, weight, *([gathered] * len(orders)))


def doppler_kernel(runs, swap_ref, high_ref, low_ref, *refs):
    ins, out_ref, turned, lines = refs[:-3], refs[-3], refs[-2], refs[-1]
    beams = out_ref.shape[0]
    blocks, parts = lines.shape[0], lines.shape[1]
    per_block = out_ref.shape[1] // blocks
    at = 0
    for first in range(0, len(ins), runs):
        slots = ins[first].shape[0]
        rows = jnp.concatenate([ref[...] for ref in ins[first : first + runs]], axis=0)
        for first in range(0, runs * slots, TILE):
            piece = rows[first : first + TILE].reshape(TILE * beams, LANES)
            piece = jnp.dot(swap_ref[...], piece, preferred_element_type=jnp.float32)
            turned[:, at : at + TILE, :] = piece.astype(jnp.bfloat16).reshape(beams, TILE, LANES)
            at += TILE
    for beam in range(beams):
        flipped = turned[beam].T
        for part in range(parts):
            for block in range(blocks):
                row = (part * blocks + block) * per_block
                lines[block, part, beam * per_block : (beam + 1) * per_block, :] = flipped[
                    row : row + per_block
                ]
    for block in range(blocks):
        total = None
        for part in range(parts):
            for table in (high_ref, low_ref):
                term = jnp.dot(
                    lines[block, part], table[block, part], preferred_element_type=jnp.float32
                )
                total = term if total is None else total + term
        count = total.shape[1] // 2
        real, imag = total[:, :count], total[:, count:]
        power = (real * real + imag * imag).reshape(beams, per_block, count)
        out_ref[:, block * per_block : (block + 1) * per_block, :] = power


def doppler(pieces, counts, high, low, per_block):
    blocks, parts, columns, width = high.shape
    runs = len(pieces[0])
    beams = pieces[0][0].shape[1]
    swap = jnp.asarray(swap_rows(TILE, TILE), jnp.bfloat16)
    whole = lambda shape: pl.BlockSpec(shape, lambda i: (0,) * len(shape))
    cells = blocks * per_block
    return pl.pallas_call(
        functools.partial(doppler_kernel, runs),
        out_shape=jax.ShapeDtypeStruct((beams, cells, width // 2), jnp.float32),
        grid=(beams // TILE,),
        in_specs=[whole(swap.shape), whole(high.shape), whole(low.shape)]
        + [
            pl.BlockSpec((slots, TILE, LANES), lambda i: (0, i, 0))
            for slots in counts
            for _ in range(runs)
        ],
        out_specs=pl.BlockSpec((TILE, cells, width // 2), lambda i: (i, 0, 0)),
        scratch_shapes=[
            pltpu.VMEM((TILE, columns, LANES), jnp.bfloat16),
            pltpu.VMEM((blocks, parts, TILE * per_block, columns), jnp.bfloat16),
        ],
        compiler_params=pltpu.CompilerParams(vmem_limit_bytes=VMEM),
        cost_estimate=pl.CostEstimate(
            flops=4 * beams * cells * parts * columns * width,
            bytes_accessed=4 * beams * cells * width,
            transcendentals=0,
        ),
        name="doppler",
    )(swap, high, low, *[piece for chunk in pieces for piece in chunk])


def add(left, right):
    return (left.astype(jnp.float32) + right.astype(jnp.float32)).astype(jnp.bfloat16)


def last_kernel(note, me_ref, *refs):
    owners, count = refs[0].shape[1:3]
    ins, outs = refs[:-owners], refs[-owners:]
    for away in range(owners):
        owner = me_ref[0] ^ away
        for half in range(2):
            total = ins[2 * half][0, owner].astype(jnp.float32)
            total = total + ins[2 * half + 1][0, owner].astype(jnp.float32)
            outs[away][half * count : (half + 1) * count] = total.astype(jnp.bfloat16)
        if note:
            outs[away][2 * count] = ins[4][...]


def last_sum(place, values, note):
    _, owners, count, beams, lanes = values[0].shape
    held = 2 * count + (0 if note is None else 1)
    extra = [] if note is None else [note]
    return pl.pallas_call(
        functools.partial(last_kernel, note is not None),
        out_shape=[jax.ShapeDtypeStruct((held, beams, lanes), jnp.bfloat16)] * owners,
        in_specs=[pl.BlockSpec(memory_space=pltpu.SMEM)]
        + [pl.BlockSpec(memory_space=pltpu.VMEM)] * (4 + len(extra)),
        out_specs=[pl.BlockSpec(memory_space=pltpu.VMEM)] * owners,
        compiler_params=pltpu.CompilerParams(vmem_limit_bytes=VMEM // 4),
        cost_estimate=pl.CostEstimate(
            flops=values[0].size * 2, bytes_accessed=values[0].size * 12, transcendentals=0
        ),
        name="last_sum",
    )(place, *values, *extra)


def per_device(echoes, keep_mask, steer_index, element_position, element_gain, steer_sines):
    groups, owners = lax.axis_size("elem"), lax.axis_size("pulse")
    _, elems, pulses, all_cells = echoes.shape
    blocks_all = keep_mask.shape[1]
    per_block = all_cells // blocks_all
    cells = all_cells // groups
    bits = groups.bit_length() - 1
    slots = (3 * pulses + 3) // 4
    me = lax.axis_index("elem")

    hit = slot_sources(keep_mask, slots)
    sources = jnp.sum(
        jnp.where(hit, jnp.arange(pulses, dtype=jnp.int32)[None, :, None], 0), axis=1
    ).reshape(-1)

    choices = jnp.arange(steer_sines.shape[0], dtype=jnp.int32)
    sines = jnp.sum(
        jnp.where(steer_index[:, None] == choices[None, :], steer_sines[None, :], 0.0),
        axis=1,
        keepdims=True,
    )
    mine = me.astype(jnp.int32).reshape(1)
    place = lax.axis_index("pulse").astype(jnp.int32).reshape(1)
    weight = local_weight(mine, element_position[None, :], element_gain, sines, elems)
    forward = tuple(range(bits))
    orders = (forward, forward[::-1])
    shares = SHARES if sum(SHARES) * 2 == slots else (1,) * (slots // 2)

    def send(value, bit):
        return lax.ppermute(value, "elem", [(i, i ^ (1 << bit)) for i in range(groups)])

    beams = weight.shape[0]
    note = jnp.pad(
        keep_mask.astype(jnp.bfloat16).reshape(-1),
        (0, beams // owners * 2 * cells - keep_mask.size),
    ).reshape(beams // owners, 2 * cells)

    head = gather_slots(echoes, sources, 0, 2 * shares[0], pulses - slots, per_block, groups)
    pieces = []
    summed = []
    first = 0
    for pair, count in enumerate(shares):
        own = weight
        if pair >= 2:
            own = lax.optimization_barrier((weight, summed[pair - 2]))[0]
        if pair == 0:
            outs = form_beams(mine, own, head, 0, count, orders, owners)
        else:
            outs = form_beams(mine, own, tail, first - 2 * shares[0], count, orders, owners)
        first += 2 * count
        if pair == 0:
            where = lax.optimization_barrier((sources, outs[1]))[0]
            tail = gather_slots(
                echoes, where, first, slots - first, pulses - slots, per_block, groups
            )
        states = [(outs[0], outs[1]), (outs[2], outs[3])]
        last = []
        for stage in range(bits):
            for half in range(2):
                keep, away = states[half]
                got = send(away, orders[half][stage])
                if stage == bits - 1:
                    last += [got, keep]
                else:
                    middle = keep.shape[0] // 2
                    states[half] = (
                        add(got[:middle], keep[:middle]),
                        add(got[middle:], keep[middle:]),
                    )
            if stage == 0:
                summed.append(jax.tree.leaves(states)[0])
        final = last_sum(place, last, note if pair == 0 else None)
        arrived = [final[0]]
        for away in range(1, owners):
            arrived.append(
                lax.ppermute(final[away], "pulse", [(i, i ^ away) for i in range(owners)])
            )
        pieces.append(arrived)

    counts = [2 * count for count in shares]
    rows = -(-keep_mask.size // LANES)
    noted = lax.optimization_barrier((pieces[0], pieces[max(len(pieces) - 2, 0)][0]))[0]
    every_mask = jnp.stack([piece[counts[0], :rows].reshape(-1) for piece in noted])
    every_mask = every_mask[:, : keep_mask.size]
    every_mask = every_mask.reshape((owners,) + keep_mask.shape).astype(jnp.int32)
    near = lax.dynamic_slice_in_dim(every_mask, me * (cells // per_block), cells // per_block, 2)
    hits = slot_sources(near, slots)
    hits = hits & (near[:, None] == 1)
    high, low = tables(P_SIZE)
    run_eye = jnp.arange(owners, dtype=jnp.int32)
    order = []
    names = []
    first = 0
    for size in counts:
        part = hits[:, first : first + size]
        order.append(part.reshape(owners * size, pulses, -1))
        names.append(jnp.repeat(run_eye ^ place[0], size))
        first += size
    picks = jnp.concatenate(order, axis=0)
    runs = jnp.concatenate(names)
    onehot = (
        (runs[:, None] == run_eye[None, :])[:, :, None, None] & picks[:, None, :, :]
    ).reshape(picks.shape[0], owners * pulses, -1).astype(jnp.bfloat16)

    def chosen(table):
        halves = table.reshape(2 * P_SIZE, 2, P_SIZE)
        return jnp.einsum(
            "fcp,spk->kcsf", halves, onehot, preferred_element_type=jnp.float32
        ).astype(jnp.bfloat16)

    pieces[0] = noted
    power = doppler(pieces, counts, chosen(high), chosen(low), per_block)
    return jnp.transpose(power, (0, 2, 1))


def solution(mesh):
    placed = (P(None, "elem", "pulse", None), P("pulse", None), P(), P(), P(), P())

    return jax.shard_map(
        per_device, mesh=mesh, in_specs=placed, out_specs=P("pulse", None, "elem"), check_vma=False
    )
```

```python
import functools
import math

import jax
import jax.numpy as jnp
import numpy as np
from jax import lax
from jax.experimental import pallas as pl
from jax.experimental.pallas import tpu as pltpu
from jax.sharding import PartitionSpec as P


E = 2048
P_SIZE = 256
LANES = 128
TILE = 16
READS = 2
VMEM = 60 * 1024 * 1024
SHARES = (4, 3, 3, 2)


def tables(count):
    index = jnp.arange(count, dtype=jnp.int32)
    angle = 2.0 * math.pi * (index[:, None] * index[None, :] % count).astype(jnp.float32) / count
    taper = 0.54 - 0.46 * jnp.cos(2.0 * math.pi * index.astype(jnp.float32) / (count - 1))
    taper = taper / math.sqrt(count)
    cos_table = jnp.cos(angle) * taper[None, :]
    sin_table = jnp.sin(angle) * taper[None, :]
    upper = jnp.concatenate((cos_table, sin_table), axis=1)
    lower = jnp.concatenate((-sin_table, cos_table), axis=1)
    transform = jnp.concatenate((upper, lower), axis=0)
    high = transform.astype(jnp.bfloat16)
    low = (transform - high.astype(jnp.float32)).astype(jnp.bfloat16)
    return (high, low)


def cos_sin(phase):
    turns = jnp.floor(phase * (2.0 / math.pi) + 0.5)
    rest = phase - turns * 1.5703125
    rest = rest - turns * 4.837512969970703e-4
    rest = rest - turns * 7.54978995489188e-8
    square = rest * rest
    sine = ((-1.9515295891e-4 * square + 8.3321608736e-3) * square - 1.6666654611e-1) * square * rest + rest
    cosine = (2.443315711809948e-5 * square - 1.388731625493765e-3) * square + 4.166664568298827e-2
    cosine = cosine * square * square - 0.5 * square + 1.0
    quadrant = turns.astype(jnp.int32)
    odd = (quadrant & 1) == 1
    real = jnp.where(odd, sine, cosine)
    imag = jnp.where(odd, cosine, sine)
    real = jnp.where(((quadrant + 1) & 2) == 2, -real, real)
    imag = jnp.where((quadrant & 2) == 2, -imag, imag)
    return (real, imag)


def weight_kernel(me_ref, sine_ref, position_ref, gain_ref, out_ref):
    phase = (2.0 * math.pi * position_ref[...]) * sine_ref[...]
    cosine, sine = cos_sin(phase)
    factor = 1.0 / math.sqrt(E)
    first, second = gain_ref[0:1, :], gain_ref[1:2, :]
    real = ((first * cosine + second * sine) * factor).astype(jnp.bfloat16)
    imag = (second * cosine - first * sine) * factor
    elems = real.shape[1]
    out_ref[:, :elems] = real
    out_ref[:, elems:] = imag.astype(jnp.bfloat16)


def local_weight(me, position, gain, sines, elems):
    beams = sines.shape[0]
    step = min(beams, 128)
    return pl.pallas_call(
        weight_kernel,
        out_shape=jax.ShapeDtypeStruct((beams, 2 * elems), jnp.bfloat16),
        grid_spec=pltpu.PrefetchScalarGridSpec(
            num_scalar_prefetch=1,
            grid=(beams // step,),
            in_specs=[
                pl.BlockSpec((step, 1), lambda i, me: (i, 0)),
                pl.BlockSpec((1, elems), lambda i, me: (0, me[0])),
                pl.BlockSpec((2, elems), lambda i, me: (0, me[0])),
            ],
            out_specs=pl.BlockSpec((step, 2 * elems), lambda i, me: (i, 0)),
        ),
        compiler_params=pltpu.CompilerParams(vmem_limit_bytes=VMEM // 4),
        cost_estimate=pl.CostEstimate(
            flops=40 * beams * elems, bytes_accessed=8 * beams * elems, transcendentals=0
        ),
        name="weights",
    )(me, sines, position, gain)


def slot_sources(mask, slots):
    length = mask.shape[-2]
    zeroed = 1 - mask
    index = jnp.arange(length, dtype=jnp.int32)
    earlier = (index[:, None] > index[None, :]).astype(jnp.int32)
    before = jnp.sum(earlier[:, :, None] * zeroed[..., None, :, :], axis=-2)
    out = (zeroed == 1) & (before < length - slots)
    rank = index[:, None] - jnp.minimum(before, length - slots)
    ids = jnp.arange(slots, dtype=jnp.int32)
    hit = (rank[..., None, :, :] == ids[:, None, None]) & jnp.logical_not(out)[..., None, :, :]
    return hit


def swap_rows(outer, inner):
    row = np.arange(outer * inner)
    return ((row % outer) * inner + row // outer)[:, None] == row[None, :]


def gather_kernel(first, count, offset, per_block, src_ref, swap_ref, *refs):
    xs, out_ref, turned = refs[:-2], refs[-2], refs[-1]
    depth, pulses, all_cells = xs[0].shape[1:]
    elems = READS * depth
    groups = out_ref.shape[1]
    cells = all_cells // groups
    rows = swap_ref.shape[0]
    estep = rows // pulses
    low = lax.broadcasted_iota(jnp.int32, (rows, LANES), 1) < cells
    for start in range(0, elems, estep):
        for at in range(len(xs) // (2 * READS)):
            real, imag = [
                jnp.dot(
                    swap_ref[...],
                    xs[(2 * at + part) * READS + start // depth][
                        0, start % depth : start % depth + estep
                    ].reshape(rows, all_cells),
                    preferred_element_type=jnp.float32,
                )
                for part in range(2)
            ]
            for column in range(all_cells // LANES):
                span = slice(column * LANES, (column + 1) * LANES)
                re, im = real[:, span], imag[:, span]
                even = jnp.where(low, re, pltpu.roll(im, cells, 1))
                odd = jnp.where(low, pltpu.roll(re, cells, 1), im)
                for side, value in enumerate((even, odd)):
                    turned[
                        at * pulses : (at + 1) * pulses, 2 * column + side, start : start + estep, :
                    ] = value.astype(jnp.bfloat16).reshape(pulses, estep, LANES)
    per_group = cells // per_block
    block = lax.broadcasted_iota(jnp.int32, (elems, LANES), 1) % cells // per_block

    def slot(s, carry):
        for group in range(groups):
            place = (first + s) * (groups * per_group) + group * per_group
            value = turned[src_ref[place] - offset, group]
            for piece in range(1, per_group):
                value = jnp.where(block >= piece, turned[src_ref[place + piece] - offset, group], value)
            out_ref[s, group] = value
        return carry

    lax.fori_loop(0, count, slot, 0)


def gather_slots(echoes, sources, first, count, spare, per_block, groups):
    parts, elems, pulses, all_cells = echoes.shape
    chunk = min(elems, 64)
    pstep = min(pulses, TILE)
    estep = TILE * TILE // pstep
    swap = jnp.asarray(swap_rows(estep, pstep), jnp.bfloat16)
    runs = range(first // pstep, (first + count - 1 + spare) // pstep + 1)
    read = echoes.size * len(runs) * pstep // pulses
    return pl.pallas_call(
        functools.partial(gather_kernel, first, count, runs[0] * pstep, per_block),
        out_shape=jax.ShapeDtypeStruct((count, groups, elems, LANES), jnp.bfloat16),
        grid_spec=pltpu.PrefetchScalarGridSpec(
            num_scalar_prefetch=1,
            grid=(elems // chunk,),
            in_specs=[pl.BlockSpec(swap.shape, lambda e, src: (0, 0))]
            + [
                pl.BlockSpec(
                    (1, chunk // READS, pstep, all_cells),
                    functools.partial(
                        lambda part, read, at, e, src: (part, READS * e + read, at, 0), part, read, run
                    ),
                )
                for run in runs
                for part in range(parts)
                for read in range(READS)
            ],
            out_specs=pl.BlockSpec((count, groups, chunk, LANES), lambda e, src: (0, 0, e, 0)),
            scratch_shapes=[pltpu.VMEM((len(runs) * pstep, groups, chunk, LANES), jnp.bfloat16)],
        ),
        compiler_params=pltpu.CompilerParams(vmem_limit_bytes=VMEM - 4 * 1024 * 1024),
        cost_estimate=pl.CostEstimate(
            flops=2 * read * TILE * TILE, bytes_accessed=4 * read, transcendentals=0
        ),
        name="gather_slots",
    )(sources, swap, *([echoes] * (len(runs) * parts * READS)))


def beam_kernel(groups, orders, me_ref, w_ref, *refs):
    xs, outs = refs[: len(orders)], refs[len(orders) :]
    bits = len(orders[0])
    elems = w_ref.shape[1] // 2
    cells = LANES // 2
    sign = jnp.where(lax.broadcasted_iota(jnp.int32, (elems, LANES), 1) < cells, -1.0, 1.0)
    sign = sign.astype(jnp.bfloat16)
    for half, order in enumerate(orders):
        plain, crossed = [], []
        for place in range(groups):
            away = 0
            for at, bit in enumerate(order):
                away |= ((place >> (bits - 1 - at)) & 1) << bit
            value = xs[half][0, me_ref[0] ^ away]
            plain.append(value)
            crossed.append(pltpu.roll(value, cells, 1) * sign)
        both = jnp.concatenate(
            (jnp.concatenate(plain, axis=1), jnp.concatenate(crossed, axis=1)), axis=0
        )
        total = jnp.dot(w_ref[...], both, preferred_element_type=jnp.float32)
        for place in range(groups):
            ref = outs[2 * half + (1 if place >= groups // 2 else 0)]
            value = total[:, place * LANES : (place + 1) * LANES].astype(jnp.bfloat16)
            ref[place % (groups // 2), :, 0] = value.reshape(ref.shape[1], ref.shape[3], LANES)


def form_beams(me, weight, gathered, first, count, orders, owners):
    _, groups, elems, lanes = gathered.shape
    beams = weight.shape[0]
    shape = (groups // 2, owners, count, beams // owners, lanes)
    block = shape[:2] + (1,) + shape[3:]
    starts = [first + half * count for half in range(len(orders))]
    outs = [jax.ShapeDtypeStruct(shape, jnp.bfloat16)] * (2 * len(orders))
    return pl.pallas_call(
        functools.partial(beam_kernel, groups, orders),
        out_shape=outs,
        grid_spec=pltpu.PrefetchScalarGridSpec(
            num_scalar_prefetch=1,
            grid=(count,),
            in_specs=[pl.BlockSpec(weight.shape, lambda i, me: (0, 0))]
            + [
                pl.BlockSpec(
                    (1, groups, elems, lanes), functools.partial(lambda at, i, me: (at + i, 0, 0, 0), at)
                )
                for at in starts
            ],
            out_specs=[pl.BlockSpec(block, lambda i, me: (0, 0, i, 0, 0))] * len(outs),
        ),
        compiler_params=pltpu.CompilerParams(vmem_limit_bytes=VMEM - 4 * 1024 * 1024),
        cost_estimate=pl.CostEstimate(
            flops=4 * len(orders) * count * weight.size * groups * lanes,
            bytes_accessed=2 * weight.size + 8 * len(orders) * count * groups * elems * lanes,
            transcendentals=0,
        ),
        name="form_beams",
    )(me, weight, *([gathered] * len(orders)))


def doppler_kernel(runs, swap_ref, high_ref, low_ref, *refs):
    ins, out_ref, turned, lines = refs[:-3], refs[-3], refs[-2], refs[-1]
    beams = out_ref.shape[0]
    blocks, parts = lines.shape[0], lines.shape[2] // turned.shape[1]
    per_block = out_ref.shape[1] // blocks
    at = 0
    for first in range(0, len(ins), runs):
        slots = ins[first].shape[0]
        rows = jnp.concatenate([ref[...] for ref in ins[first : first + runs]], axis=0)
        for first in range(0, runs * slots, TILE):
            piece = rows[first : first + TILE].reshape(TILE * beams, LANES)
            piece = jnp.dot(swap_ref[...], piece, preferred_element_type=jnp.float32)
            turned[:, at : at + TILE, :] = piece.astype(jnp.bfloat16).reshape(beams, TILE, LANES)
            at += TILE

    @pl.when(pl.program_id(0) == 0)
    def _():
        turned[:, at:, :] = jnp.zeros((beams, turned.shape[1] - at, LANES), jnp.bfloat16)

    width = turned.shape[1]
    for beam in range(beams):
        flipped = turned[beam].T
        for part in range(parts):
            for block in range(blocks):
                row = (part * blocks + block) * per_block
                lines[
                    block, beam * per_block : (beam + 1) * per_block, part * width : (part + 1) * width
                ] = flipped[row : row + per_block]
    for block in range(blocks):
        total = jnp.dot(lines[block], high_ref[block], preferred_element_type=jnp.float32)
        total = total + jnp.dot(lines[block], low_ref[block], preferred_element_type=jnp.float32)
        count = total.shape[1] // 2
        real, imag = total[:, :count], total[:, count:]
        power = (real * real + imag * imag).reshape(beams, per_block, count)
        out_ref[:, block * per_block : (block + 1) * per_block, :] = power


def doppler(pieces, counts, high, low, per_block):
    blocks, parts, columns, width = high.shape
    runs = len(pieces[0])
    beams = pieces[0][0].shape[1]
    swap = jnp.asarray(swap_rows(TILE, TILE), jnp.bfloat16)
    whole = lambda shape: pl.BlockSpec(shape, lambda i: (0,) * len(shape))
    cells = blocks * per_block
    return pl.pallas_call(
        functools.partial(doppler_kernel, runs),
        out_shape=jax.ShapeDtypeStruct((beams, cells, width // 2), jnp.float32),
        grid=(beams // TILE,),
        in_specs=[whole(swap.shape), whole((blocks, parts * columns, width)), whole((blocks, parts * columns, width))]
        + [
            pl.BlockSpec((slots, TILE, LANES), lambda i: (0, i, 0))
            for slots in counts
            for _ in range(runs)
        ],
        out_specs=pl.BlockSpec((TILE, cells, width // 2), lambda i: (i, 0, 0)),
        scratch_shapes=[
            pltpu.VMEM((TILE, columns, LANES), jnp.bfloat16),
            pltpu.VMEM((blocks, TILE * per_block, parts * columns), jnp.bfloat16),
        ],
        compiler_params=pltpu.CompilerParams(vmem_limit_bytes=VMEM),
        cost_estimate=pl.CostEstimate(
            flops=4 * beams * cells * parts * columns * width,
            bytes_accessed=4 * beams * cells * width,
            transcendentals=0,
        ),
        name="doppler",
    )(
        swap,
        high.reshape(blocks, parts * columns, width),
        low.reshape(blocks, parts * columns, width),
        *[piece for chunk in pieces for piece in chunk],
    )


def add(left, right):
    return (left.astype(jnp.float32) + right.astype(jnp.float32)).astype(jnp.bfloat16)


def last_kernel(note, me_ref, *refs):
    owners, count = refs[0].shape[1:3]
    ins, outs = refs[:-owners], refs[-owners:]
    for away in range(owners):
        owner = me_ref[0] ^ away
        for half in range(2):
            total = ins[2 * half][0, owner].astype(jnp.float32)
            total = total + ins[2 * half + 1][0, owner].astype(jnp.float32)
            outs[away][half * count : (half + 1) * count] = total.astype(jnp.bfloat16)
        if note:
            outs[away][2 * count] = ins[4][...]


def last_sum(place, values, note):
    _, owners, count, beams, lanes = values[0].shape
    held = 2 * count + (0 if note is None else 1)
    extra = [] if note is None else [note]
    return pl.pallas_call(
        functools.partial(last_kernel, note is not None),
        out_shape=[jax.ShapeDtypeStruct((held, beams, lanes), jnp.bfloat16)] * owners,
        in_specs=[pl.BlockSpec(memory_space=pltpu.SMEM)]
        + [pl.BlockSpec(memory_space=pltpu.VMEM)] * (4 + len(extra)),
        out_specs=[pl.BlockSpec(memory_space=pltpu.VMEM)] * owners,
        compiler_params=pltpu.CompilerParams(vmem_limit_bytes=VMEM // 4),
        cost_estimate=pl.CostEstimate(
            flops=values[0].size * 2, bytes_accessed=values[0].size * 12, transcendentals=0
        ),
        name="last_sum",
    )(place, *values, *extra)


def collect_kernel(*refs):
    for run, ref in enumerate(refs[:-1]):
        refs[-1][run] = ref[0]


def collect(pieces, slot):
    lanes = pieces[0].shape[2]
    return pl.pallas_call(
        collect_kernel,
        out_shape=jax.ShapeDtypeStruct((len(pieces), TILE, lanes), jnp.bfloat16),
        grid=(1,),
        in_specs=[pl.BlockSpec((1, TILE, lanes), lambda i: (slot, 0, 0))] * len(pieces),
        out_specs=pl.BlockSpec((len(pieces), TILE, lanes), lambda i: (0, 0, 0)),
        compiler_params=pltpu.CompilerParams(vmem_limit_bytes=VMEM // 4),
        name="collect",
    )(*pieces)


def per_device(echoes, keep_mask, steer_index, element_position, element_gain, steer_sines):
    groups, owners = lax.axis_size("elem"), lax.axis_size("pulse")
    _, elems, pulses, all_cells = echoes.shape
    blocks_all = keep_mask.shape[1]
    per_block = all_cells // blocks_all
    cells = all_cells // groups
    bits = groups.bit_length() - 1
    slots = (3 * pulses + 3) // 4
    me = lax.axis_index("elem")

    hit = slot_sources(keep_mask, slots)
    sources = jnp.sum(
        jnp.where(hit, jnp.arange(pulses, dtype=jnp.int32)[None, :, None], 0), axis=1
    ).reshape(-1)

    choices = jnp.arange(steer_sines.shape[0], dtype=jnp.int32)
    sines = jnp.sum(
        jnp.where(steer_index[:, None] == choices[None, :], steer_sines[None, :], 0.0),
        axis=1,
        keepdims=True,
    )
    mine = me.astype(jnp.int32).reshape(1)
    place = lax.axis_index("pulse").astype(jnp.int32).reshape(1)
    weight = local_weight(mine, element_position[None, :], element_gain, sines, elems)
    forward = tuple(range(bits))
    orders = (forward, forward[::-1])
    shares = SHARES if sum(SHARES) * 2 == slots else (1,) * (slots // 2)

    def send(value, bit):
        return lax.ppermute(value, "elem", [(i, i ^ (1 << bit)) for i in range(groups)])

    beams = weight.shape[0]
    note = jnp.pad(
        keep_mask.astype(jnp.bfloat16).reshape(-1),
        (0, beams // owners * 2 * cells - keep_mask.size),
    ).reshape(beams // owners, 2 * cells)

    head = gather_slots(echoes, sources, 0, 2 * shares[0], pulses - slots, per_block, groups)
    pieces = []
    summed = []
    first = 0
    for pair, count in enumerate(shares):
        own = weight
        if pair >= 2:
            own = lax.optimization_barrier((weight, summed[pair - 2]))[0]
        if pair == 0:
            outs = form_beams(mine, own, head, 0, count, orders, owners)
        else:
            outs = form_beams(mine, own, tail, first - 2 * shares[0], count, orders, owners)
        first += 2 * count
        if pair == 0:
            where = lax.optimization_barrier((sources, outs[1]))[0]
            tail = gather_slots(
                echoes, where, first, slots - first, pulses - slots, per_block, groups
            )
        states = [(outs[0], outs[1]), (outs[2], outs[3])]
        last = []
        for stage in range(bits):
            for half in range(2):
                keep, away = states[half]
                got = send(away, orders[half][stage])
                if stage == bits - 1:
                    last += [got, keep]
                else:
                    middle = keep.shape[0] // 2
                    states[half] = (
                        add(got[:middle], keep[:middle]),
                        add(got[middle:], keep[middle:]),
                    )
            if stage == 0:
                summed.append(jax.tree.leaves(states)[0])
        final = last_sum(place, last, note if pair == 0 else None)
        arrived = [final[0]]
        for away in range(1, owners):
            arrived.append(
                lax.ppermute(final[away], "pulse", [(i, i ^ away) for i in range(owners)])
            )
        pieces.append(arrived)

    counts = [2 * count for count in shares]
    rows = -(-keep_mask.size // LANES)
    every_mask = collect(pieces[0], counts[0])[:, :rows].reshape(owners, rows * LANES)
    every_mask = every_mask[:, : keep_mask.size]
    every_mask = every_mask.reshape((owners,) + keep_mask.shape).astype(jnp.int32)
    near = lax.dynamic_slice_in_dim(every_mask, me * (cells // per_block), cells // per_block, 2)
    hits = slot_sources(near, slots)
    hits = hits & (near[:, None] == 1)
    high, low = tables(P_SIZE)
    run_eye = jnp.arange(owners, dtype=jnp.int32)
    order = []
    names = []
    first = 0
    for size in counts:
        part = hits[:, first : first + size]
        order.append(part.reshape(owners * size, pulses, -1))
        names.append(jnp.repeat(run_eye ^ place[0], size))
        first += size
    picks = jnp.concatenate(order, axis=0)
    spare = -picks.shape[0] % 256
    picks = jnp.pad(picks, ((0, spare), (0, 0), (0, 0)))
    runs = jnp.pad(jnp.concatenate(names), (0, spare))
    onehot = (
        (runs[:, None] == run_eye[None, :])[:, :, None, None] & picks[:, None, :, :]
    ).reshape(picks.shape[0], owners * pulses, -1).astype(jnp.bfloat16)

    def chosen(table):
        halves = table.reshape(2 * P_SIZE, 2, P_SIZE)
        return jnp.einsum(
            "fcp,spk->kcsf", halves, onehot, preferred_element_type=jnp.float32
        ).astype(jnp.bfloat16)

    power = doppler(pieces, counts, chosen(high), chosen(low), per_block)
    return jnp.transpose(power, (0, 2, 1))


def solution(mesh):
    placed = (P(None, "elem", "pulse", None), P("pulse", None), P(), P(), P(), P())

    return jax.shard_map(
        per_device, mesh=mesh, in_specs=placed, out_specs=P("pulse", None, "elem"), check_vma=False
    )
```

```python
import functools
import math

import jax
import jax.numpy as jnp
import numpy as np
from jax import lax
from jax.experimental import pallas as pl
from jax.experimental.pallas import tpu as pltpu
from jax.sharding import PartitionSpec as P


E = 2048
P_SIZE = 256
LANES = 128
TILE = 16
READS = 2
VMEM = 60 * 1024 * 1024
SHARES = (4, 3, 3, 2)


def tables(count):
    index = jnp.arange(count, dtype=jnp.int32)
    angle = 2.0 * math.pi * (index[:, None] * index[None, :] % count).astype(jnp.float32) / count
    taper = 0.54 - 0.46 * jnp.cos(2.0 * math.pi * index.astype(jnp.float32) / (count - 1))
    taper = taper / math.sqrt(count)
    cos_table = jnp.cos(angle) * taper[None, :]
    sin_table = jnp.sin(angle) * taper[None, :]
    upper = jnp.concatenate((cos_table, sin_table), axis=1)
    lower = jnp.concatenate((-sin_table, cos_table), axis=1)
    transform = jnp.concatenate((upper, lower), axis=0)
    high = transform.astype(jnp.bfloat16)
    low = (transform - high.astype(jnp.float32)).astype(jnp.bfloat16)
    return (high, low)


def cos_sin(phase):
    turns = jnp.floor(phase * (2.0 / math.pi) + 0.5)
    rest = phase - turns * 1.5703125
    rest = rest - turns * 4.837512969970703e-4
    rest = rest - turns * 7.54978995489188e-8
    square = rest * rest
    sine = ((-1.9515295891e-4 * square + 8.3321608736e-3) * square - 1.6666654611e-1) * square * rest + rest
    cosine = (2.443315711809948e-5 * square - 1.388731625493765e-3) * square + 4.166664568298827e-2
    cosine = cosine * square * square - 0.5 * square + 1.0
    quadrant = turns.astype(jnp.int32)
    odd = (quadrant & 1) == 1
    real = jnp.where(odd, sine, cosine)
    imag = jnp.where(odd, cosine, sine)
    real = jnp.where(((quadrant + 1) & 2) == 2, -real, real)
    imag = jnp.where((quadrant & 2) == 2, -imag, imag)
    return (real, imag)


def weight_kernel(me_ref, sine_ref, position_ref, gain_ref, out_ref):
    phase = (2.0 * math.pi * position_ref[...]) * sine_ref[...]
    cosine, sine = cos_sin(phase)
    factor = 1.0 / math.sqrt(E)
    first, second = gain_ref[0:1, :], gain_ref[1:2, :]
    real = ((first * cosine + second * sine) * factor).astype(jnp.bfloat16)
    imag = (second * cosine - first * sine) * factor
    elems = real.shape[1]
    out_ref[:, :elems] = real
    out_ref[:, elems:] = imag.astype(jnp.bfloat16)


def local_weight(me, position, gain, sines, elems):
    beams = sines.shape[0]
    step = min(beams, 128)
    return pl.pallas_call(
        weight_kernel,
        out_shape=jax.ShapeDtypeStruct((beams, 2 * elems), jnp.bfloat16),
        grid_spec=pltpu.PrefetchScalarGridSpec(
            num_scalar_prefetch=1,
            grid=(beams // step,),
            in_specs=[
                pl.BlockSpec((step, 1), lambda i, me: (i, 0)),
                pl.BlockSpec((1, elems), lambda i, me: (0, me[0])),
                pl.BlockSpec((2, elems), lambda i, me: (0, me[0])),
            ],
            out_specs=pl.BlockSpec((step, 2 * elems), lambda i, me: (i, 0)),
        ),
        compiler_params=pltpu.CompilerParams(vmem_limit_bytes=VMEM // 4),
        cost_estimate=pl.CostEstimate(
            flops=40 * beams * elems, bytes_accessed=8 * beams * elems, transcendentals=0
        ),
        name="weights",
    )(me, sines, position, gain)


def slot_sources(mask, slots):
    length = mask.shape[-2]
    zeroed = 1 - mask
    index = jnp.arange(length, dtype=jnp.int32)
    earlier = (index[:, None] > index[None, :]).astype(jnp.int32)
    before = jnp.sum(earlier[:, :, None] * zeroed[..., None, :, :], axis=-2)
    out = (zeroed == 1) & (before < length - slots)
    rank = index[:, None] - jnp.minimum(before, length - slots)
    ids = jnp.arange(slots, dtype=jnp.int32)
    hit = (rank[..., None, :, :] == ids[:, None, None]) & jnp.logical_not(out)[..., None, :, :]
    return hit


def swap_rows(outer, inner):
    row = np.arange(outer * inner)
    return ((row % outer) * inner + row // outer)[:, None] == row[None, :]


def gather_kernel(first, count, offset, per_block, src_ref, swap_ref, *refs):
    xs, out_ref, turned = refs[:-2], refs[-2], refs[-1]
    depth, pulses, all_cells = xs[0].shape[1:]
    elems = READS * depth
    groups = out_ref.shape[1]
    cells = all_cells // groups
    rows = swap_ref.shape[0]
    estep = rows // pulses
    low = lax.broadcasted_iota(jnp.int32, (rows, LANES), 1) < cells
    for start in range(0, elems, estep):
        for at in range(len(xs) // (2 * READS)):
            real, imag = [
                jnp.dot(
                    swap_ref[...],
                    xs[(2 * at + part) * READS + start // depth][
                        0, start % depth : start % depth + estep
                    ].reshape(rows, all_cells),
                    preferred_element_type=jnp.float32,
                )
                for part in range(2)
            ]
            for column in range(all_cells // LANES):
                span = slice(column * LANES, (column + 1) * LANES)
                re, im = real[:, span], imag[:, span]
                even = jnp.where(low, re, pltpu.roll(im, cells, 1))
                odd = jnp.where(low, pltpu.roll(re, cells, 1), im)
                for side, value in enumerate((even, odd)):
                    turned[
                        at * pulses : (at + 1) * pulses, 2 * column + side, start : start + estep, :
                    ] = value.astype(jnp.bfloat16).reshape(pulses, estep, LANES)
    per_group = cells // per_block
    block = lax.broadcasted_iota(jnp.int32, (elems, LANES), 1) % cells // per_block

    def slot(s, carry):
        for group in range(groups):
            place = (first + s) * (groups * per_group) + group * per_group
            value = turned[src_ref[place] - offset, group]
            for piece in range(1, per_group):
                value = jnp.where(block >= piece, turned[src_ref[place + piece] - offset, group], value)
            out_ref[s, group] = value
        return carry

    lax.fori_loop(0, count, slot, 0)


def gather_slots(echoes, sources, first, count, spare, per_block, groups):
    parts, elems, pulses, all_cells = echoes.shape
    chunk = min(elems, 64)
    pstep = min(pulses, TILE)
    estep = TILE * TILE // pstep
    swap = jnp.asarray(swap_rows(estep, pstep), jnp.bfloat16)
    runs = range(first // pstep, (first + count - 1 + spare) // pstep + 1)
    read = echoes.size * len(runs) * pstep // pulses
    return pl.pallas_call(
        functools.partial(gather_kernel, first, count, runs[0] * pstep, per_block),
        out_shape=jax.ShapeDtypeStruct((count, groups, elems, LANES), jnp.bfloat16),
        grid_spec=pltpu.PrefetchScalarGridSpec(
            num_scalar_prefetch=1,
            grid=(elems // chunk,),
            in_specs=[pl.BlockSpec(swap.shape, lambda e, src: (0, 0))]
            + [
                pl.BlockSpec(
                    (1, chunk // READS, pstep, all_cells),
                    functools.partial(
                        lambda part, read, at, e, src: (part, READS * e + read, at, 0), part, read, run
                    ),
                )
                for run in runs
                for part in range(parts)
                for read in range(READS)
            ],
            out_specs=pl.BlockSpec((count, groups, chunk, LANES), lambda e, src: (0, 0, e, 0)),
            scratch_shapes=[pltpu.VMEM((len(runs) * pstep, groups, chunk, LANES), jnp.bfloat16)],
        ),
        compiler_params=pltpu.CompilerParams(vmem_limit_bytes=VMEM - 4 * 1024 * 1024),
        cost_estimate=pl.CostEstimate(
            flops=2 * read * TILE * TILE, bytes_accessed=4 * read, transcendentals=0
        ),
        name="gather_slots",
    )(sources, swap, *([echoes] * (len(runs) * parts * READS)))


def beam_kernel(groups, orders, me_ref, w_ref, *refs):
    xs, outs = refs[: len(orders)], refs[len(orders) :]
    bits = len(orders[0])
    elems = w_ref.shape[1] // 2
    cells = LANES // 2
    sign = jnp.where(lax.broadcasted_iota(jnp.int32, (elems, LANES), 1) < cells, -1.0, 1.0)
    sign = sign.astype(jnp.bfloat16)
    for half, order in enumerate(orders):
        plain, crossed = [], []
        for place in range(groups):
            away = 0
            for at, bit in enumerate(order):
                away |= ((place >> (bits - 1 - at)) & 1) << bit
            value = xs[half][0, me_ref[0] ^ away]
            plain.append(value)
            crossed.append(pltpu.roll(value, cells, 1) * sign)
        both = jnp.concatenate(
            (jnp.concatenate(plain, axis=1), jnp.concatenate(crossed, axis=1)), axis=0
        )
        total = jnp.dot(w_ref[...], both, preferred_element_type=jnp.float32)
        for place in range(groups):
            ref = outs[2 * half + (1 if place >= groups // 2 else 0)]
            value = total[:, place * LANES : (place + 1) * LANES].astype(jnp.bfloat16)
            ref[place % (groups // 2), :, 0] = value.reshape(ref.shape[1], ref.shape[3], LANES)


def form_beams(me, weight, gathered, first, count, orders, owners):
    _, groups, elems, lanes = gathered.shape
    beams = weight.shape[0]
    shape = (groups // 2, owners, count, beams // owners, lanes)
    block = shape[:2] + (1,) + shape[3:]
    starts = [first + half * count for half in range(len(orders))]
    outs = [jax.ShapeDtypeStruct(shape, jnp.bfloat16)] * (2 * len(orders))
    return pl.pallas_call(
        functools.partial(beam_kernel, groups, orders),
        out_shape=outs,
        grid_spec=pltpu.PrefetchScalarGridSpec(
            num_scalar_prefetch=1,
            grid=(count,),
            in_specs=[pl.BlockSpec(weight.shape, lambda i, me: (0, 0))]
            + [
                pl.BlockSpec(
                    (1, groups, elems, lanes), functools.partial(lambda at, i, me: (at + i, 0, 0, 0), at)
                )
                for at in starts
            ],
            out_specs=[pl.BlockSpec(block, lambda i, me: (0, 0, i, 0, 0))] * len(outs),
        ),
        compiler_params=pltpu.CompilerParams(vmem_limit_bytes=VMEM - 4 * 1024 * 1024),
        cost_estimate=pl.CostEstimate(
            flops=4 * len(orders) * count * weight.size * groups * lanes,
            bytes_accessed=2 * weight.size + 8 * len(orders) * count * groups * elems * lanes,
            transcendentals=0,
        ),
        name="form_beams",
    )(me, weight, *([gathered] * len(orders)))


def doppler_kernel(runs, last, prior, swap_ref, high_ref, low_ref, *refs):
    ins, out_ref, turned, lines = refs[:-3], refs[-3], refs[-2], refs[-1]
    if prior:
        prior_ref, ins = ins[0], ins[1:]
    beams = out_ref.shape[0]
    blocks, parts = lines.shape[0], lines.shape[2] // turned.shape[1]
    per_block = out_ref.shape[1] // blocks
    at = 0
    for first in range(0, len(ins), runs):
        slots = ins[first].shape[0]
        rows = jnp.concatenate([ref[...] for ref in ins[first : first + runs]], axis=0)
        for first in range(0, runs * slots, TILE):
            piece = rows[first : first + TILE].reshape(TILE * beams, LANES)
            piece = jnp.dot(swap_ref[...], piece, preferred_element_type=jnp.float32)
            turned[:, at : at + TILE, :] = piece.astype(jnp.bfloat16).reshape(beams, TILE, LANES)
            at += TILE

    if at < turned.shape[1]:

        @pl.when(pl.program_id(0) == 0)
        def _():
            turned[:, at:, :] = jnp.zeros((beams, turned.shape[1] - at, LANES), jnp.bfloat16)

    width = turned.shape[1]
    for beam in range(beams):
        flipped = turned[beam].T
        for part in range(parts):
            for block in range(blocks):
                row = (part * blocks + block) * per_block
                lines[
                    block, beam * per_block : (beam + 1) * per_block, part * width : (part + 1) * width
                ] = flipped[row : row + per_block]
    for block in range(blocks):
        total = jnp.dot(lines[block], high_ref[block], preferred_element_type=jnp.float32)
        total = total + jnp.dot(lines[block], low_ref[block], preferred_element_type=jnp.float32)
        cells = slice(block * per_block, (block + 1) * per_block)
        total = total.reshape(beams, per_block, total.shape[1])
        if prior:
            total = total + prior_ref[:, cells, :]
        if last:
            count = total.shape[2] // 2
            real, imag = total[..., :count], total[..., count:]
            out_ref[:, cells, :] = real * real + imag * imag
        else:
            out_ref[:, cells, :] = total


def doppler(pieces, counts, high, low, per_block, prior, last):
    blocks, parts, columns, width = high.shape
    runs = len(pieces[0])
    beams = pieces[0][0].shape[1]
    swap = jnp.asarray(swap_rows(TILE, TILE), jnp.bfloat16)
    whole = lambda shape: pl.BlockSpec(shape, lambda i: (0,) * len(shape))
    cells = blocks * per_block
    bins = width // 2 if last else width
    held = [] if prior is None else [prior]
    return pl.pallas_call(
        functools.partial(doppler_kernel, runs, last, prior is not None),
        out_shape=jax.ShapeDtypeStruct((beams, cells, bins), jnp.float32),
        grid=(beams // TILE,),
        in_specs=[whole(swap.shape), whole((blocks, parts * columns, width)), whole((blocks, parts * columns, width))]
        + [pl.BlockSpec((TILE, cells, width), lambda i: (i, 0, 0))] * len(held)
        + [
            pl.BlockSpec((slots, TILE, LANES), lambda i: (0, i, 0))
            for slots in counts
            for _ in range(runs)
        ],
        out_specs=pl.BlockSpec((TILE, cells, bins), lambda i: (i, 0, 0)),
        scratch_shapes=[
            pltpu.VMEM((TILE, columns, LANES), jnp.bfloat16),
            pltpu.VMEM((blocks, TILE * per_block, parts * columns), jnp.bfloat16),
        ],
        compiler_params=pltpu.CompilerParams(vmem_limit_bytes=VMEM),
        cost_estimate=pl.CostEstimate(
            flops=4 * beams * cells * parts * columns * width,
            bytes_accessed=4 * beams * cells * width,
            transcendentals=0,
        ),
        name="doppler",
    )(
        swap,
        high.reshape(blocks, parts * columns, width),
        low.reshape(blocks, parts * columns, width),
        *held,
        *[piece for chunk in pieces for piece in chunk],
    )


def add(left, right):
    return (left.astype(jnp.float32) + right.astype(jnp.float32)).astype(jnp.bfloat16)


def last_kernel(note, me_ref, *refs):
    owners, count = refs[0].shape[1:3]
    ins, outs = refs[:-owners], refs[-owners:]
    for away in range(owners):
        owner = me_ref[0] ^ away
        for half in range(2):
            total = ins[2 * half][0, owner].astype(jnp.float32)
            total = total + ins[2 * half + 1][0, owner].astype(jnp.float32)
            outs[away][half * count : (half + 1) * count] = total.astype(jnp.bfloat16)
        if note:
            outs[away][2 * count] = ins[4][...]


def last_sum(place, values, note):
    _, owners, count, beams, lanes = values[0].shape
    held = 2 * count + (0 if note is None else 1)
    extra = [] if note is None else [note]
    return pl.pallas_call(
        functools.partial(last_kernel, note is not None),
        out_shape=[jax.ShapeDtypeStruct((held, beams, lanes), jnp.bfloat16)] * owners,
        in_specs=[pl.BlockSpec(memory_space=pltpu.SMEM)]
        + [pl.BlockSpec(memory_space=pltpu.VMEM)] * (4 + len(extra)),
        out_specs=[pl.BlockSpec(memory_space=pltpu.VMEM)] * owners,
        compiler_params=pltpu.CompilerParams(vmem_limit_bytes=VMEM // 4),
        cost_estimate=pl.CostEstimate(
            flops=values[0].size * 2, bytes_accessed=values[0].size * 12, transcendentals=0
        ),
        name="last_sum",
    )(place, *values, *extra)


def collect_kernel(*refs):
    for run, ref in enumerate(refs[:-1]):
        refs[-1][run] = ref[0]


def collect(pieces, slot):
    lanes = pieces[0].shape[2]
    return pl.pallas_call(
        collect_kernel,
        out_shape=jax.ShapeDtypeStruct((len(pieces), TILE, lanes), jnp.bfloat16),
        grid=(1,),
        in_specs=[pl.BlockSpec((1, TILE, lanes), lambda i: (slot, 0, 0))] * len(pieces),
        out_specs=pl.BlockSpec((len(pieces), TILE, lanes), lambda i: (0, 0, 0)),
        compiler_params=pltpu.CompilerParams(vmem_limit_bytes=VMEM // 4),
        name="collect",
    )(*pieces)


def per_device(echoes, keep_mask, steer_index, element_position, element_gain, steer_sines):
    groups, owners = lax.axis_size("elem"), lax.axis_size("pulse")
    _, elems, pulses, all_cells = echoes.shape
    blocks_all = keep_mask.shape[1]
    per_block = all_cells // blocks_all
    cells = all_cells // groups
    bits = groups.bit_length() - 1
    slots = (3 * pulses + 3) // 4
    me = lax.axis_index("elem")

    hit = slot_sources(keep_mask, slots)
    sources = jnp.sum(
        jnp.where(hit, jnp.arange(pulses, dtype=jnp.int32)[None, :, None], 0), axis=1
    ).reshape(-1)

    choices = jnp.arange(steer_sines.shape[0], dtype=jnp.int32)
    sines = jnp.sum(
        jnp.where(steer_index[:, None] == choices[None, :], steer_sines[None, :], 0.0),
        axis=1,
        keepdims=True,
    )
    mine = me.astype(jnp.int32).reshape(1)
    place = lax.axis_index("pulse").astype(jnp.int32).reshape(1)
    weight = local_weight(mine, element_position[None, :], element_gain, sines, elems)
    forward = tuple(range(bits))
    orders = (forward, forward[::-1])
    shares = SHARES if sum(SHARES) * 2 == slots else (1,) * (slots // 2)

    def send(value, bit):
        return lax.ppermute(value, "elem", [(i, i ^ (1 << bit)) for i in range(groups)])

    beams = weight.shape[0]
    note = jnp.pad(
        keep_mask.astype(jnp.bfloat16).reshape(-1),
        (0, beams // owners * 2 * cells - keep_mask.size),
    ).reshape(beams // owners, 2 * cells)

    head = gather_slots(echoes, sources, 0, 2 * shares[0], pulses - slots, per_block, groups)
    pieces = []
    summed = []
    first = 0
    for pair, count in enumerate(shares):
        own = weight
        if pair >= 2:
            own = lax.optimization_barrier((weight, summed[pair - 2]))[0]
        if pair == 0:
            outs = form_beams(mine, own, head, 0, count, orders, owners)
        else:
            outs = form_beams(mine, own, tail, first - 2 * shares[0], count, orders, owners)
        first += 2 * count
        if pair == 0:
            where = lax.optimization_barrier((sources, outs[1]))[0]
            tail = gather_slots(
                echoes, where, first, slots - first, pulses - slots, per_block, groups
            )
        states = [(outs[0], outs[1]), (outs[2], outs[3])]
        last = []
        for stage in range(bits):
            for half in range(2):
                keep, away = states[half]
                got = send(away, orders[half][stage])
                if stage == bits - 1:
                    last += [got, keep]
                else:
                    middle = keep.shape[0] // 2
                    states[half] = (
                        add(got[:middle], keep[:middle]),
                        add(got[middle:], keep[middle:]),
                    )
            if stage == 0:
                summed.append(jax.tree.leaves(states)[0])
        final = last_sum(place, last, note if pair == 0 else None)
        arrived = [final[0]]
        for away in range(1, owners):
            arrived.append(
                lax.ppermute(final[away], "pulse", [(i, i ^ away) for i in range(owners)])
            )
        pieces.append(arrived)

    counts = [2 * count for count in shares]
    rows = -(-keep_mask.size // LANES)
    every_mask = collect(pieces[0], counts[0])[:, :rows].reshape(owners, rows * LANES)
    every_mask = every_mask[:, : keep_mask.size]
    every_mask = every_mask.reshape((owners,) + keep_mask.shape).astype(jnp.int32)
    near = lax.dynamic_slice_in_dim(every_mask, me * (cells // per_block), cells // per_block, 2)
    hits = slot_sources(near, slots)
    hits = hits & (near[:, None] == 1)
    high, low = tables(P_SIZE)
    run_eye = jnp.arange(owners, dtype=jnp.int32)

    def chosen(first, last):
        order, names = [], []
        for pair in range(first, last):
            size, at = counts[pair], sum(counts[:pair])
            order.append(hits[:, at : at + size].reshape(owners * size, pulses, -1))
            names.append(jnp.repeat(run_eye ^ place[0], size))
        picks = jnp.concatenate(order, axis=0)
        spare = -picks.shape[0] % LANES
        picks = jnp.pad(picks, ((0, spare), (0, 0), (0, 0)))
        runs = jnp.pad(jnp.concatenate(names), (0, spare))
        onehot = (
            (runs[:, None] == run_eye[None, :])[:, :, None, None] & picks[:, None, :, :]
        ).reshape(picks.shape[0], owners * pulses, -1).astype(jnp.bfloat16)
        return [
            jnp.einsum(
                "fcp,spk->kcsf",
                table.reshape(2 * P_SIZE, 2, P_SIZE),
                onehot,
                preferred_element_type=jnp.float32,
            ).astype(jnp.bfloat16)
            for table in (high, low)
        ]

    pairs = len(counts)
    partial = doppler(
        pieces[:-1], counts[:-1], *chosen(0, pairs - 1), per_block, None, False
    )
    power = doppler(pieces[-1:], counts[-1:], *chosen(pairs - 1, pairs), per_block, partial, True)
    return jnp.transpose(power, (0, 2, 1))


def solution(mesh):
    placed = (P(None, "elem", "pulse", None), P("pulse", None), P(), P(), P(), P())

    return jax.shard_map(
        per_device, mesh=mesh, in_specs=placed, out_specs=P("pulse", None, "elem"), check_vma=False
    )
```
